128 devices in a mesh: grp: 16 (over z, y), mem: 8 (over x, core).
Axes of the slice: x: 4, y: 4, z: 4, core: 2. Of those that a mesh axis runs over, the one named last changes fastest.
Arguments:
- queries: bfloat16 [32768, 2048], P(('grp', 'mem')), may hold values from -6 to 6
- keys: bfloat16 [32768, 2048], P(('grp', 'mem')), may hold values from -6 to 6
- values: bfloat16 [32768, 2048], P(('grp', 'mem')), may hold values from -6 to 6
- grad_out: bfloat16 [32768, 2048], P(('grp', 'mem')), may hold values from -0.0625 to 0.0625
- log_decay: float32 [8, 32768], P(None, ('grp', 'mem')), may hold values from -1.6 to 0
Outputs:
- grad_queries: bfloat16 [32768, 2048], P(('grp', 'mem'))
- grad_keys: bfloat16 [32768, 2048], P(('grp', 'mem'))
- grad_values: bfloat16 [32768, 2048], P(('grp', 'mem'))
The draws below stay inside these ranges and needn't reach their ends.
All inputs are finite; a program needn't handle non-finite values.
Results may differ from the reference program's by a relative error of at most 0.0052.
Values sent between devices are 32-bit elements; how exact they have to be, the bound alone decides.
No kernel may reach another device: no remote copies, remote signals or barrier semaphores. Data moves between devices by JAX's collectives and lax.ppermute only.
A program may use at most 128 MiB of HBM per device.

```python
import jax
import jax.numpy as jnp
from jax import lax

HEAD_COUNT = 8
DK = 256
DV = 256
BLOCK = 128
TOK_DEV = 256
SEQUENCE_TOKENS = 32768


def draw_log_decay(key, part):
    base_key = jax.random.fold_in(key, 7)
    key_collection = jax.random.split(base_key, 6)
    order = jax.random.permutation(key_collection[0], HEAD_COUNT)
    fast_count = HEAD_COUNT // 2
    fast = order < fast_count
    fast_rate = jnp.exp(jax.random.uniform(key_collection[1], (HEAD_COUNT,), jnp.float32, jnp.log(1.0 / 50.0), jnp.log(1.0 / 30.0)))
    slow_rate = 0.3 / SEQUENCE_TOKENS
    decay_rates = jnp.where(fast, fast_rate, slow_rate)
    approximate = jnp.exp(jax.random.uniform(key_collection[2], (HEAD_COUNT, SEQUENCE_TOKENS), jnp.float32, jnp.log(0.5), jnp.log(2.0)))
    device_count = SEQUENCE_TOKENS // TOK_DEV
    device_factor = jnp.exp(jax.random.uniform(key_collection[3], (HEAD_COUNT, device_count), jnp.float32, jnp.log(0.5), jnp.log(2.0)))
    device_complete = jnp.repeat(device_factor, TOK_DEV, axis=1)
    spike_start = jax.random.randint(key_collection[4], (HEAD_COUNT, 2), 0, SEQUENCE_TOKENS)
    spike_length = jax.random.uniform(key_collection[5], (HEAD_COUNT, 2), jnp.float32, 0.22, 0.69)
    token_positions = jnp.arange(SEQUENCE_TOKENS)
    match_count = (token_positions[None, None, :] == spike_start[:, :, None]).astype(jnp.float32)
    spike_run = jnp.sum(match_count * spike_length[:, :, None], axis=1)
    return (-(decay_rates[:, None] * approximate * device_complete) - spike_run).astype(jnp.float32)


def block_levels(key, shape, cuts, least, high):
    level = 1.0
    for axis_at, parts in cuts:
        steps = jax.random.uniform(jax.random.fold_in(jax.random.fold_in(key, 6), axis_at), (parts,), jnp.float32, least / len(cuts), high / len(cuts))
        level = level * jnp.repeat(jnp.exp(steps), shape[axis_at] // parts).reshape((-1,) + (1,) * (len(shape) - 1 - axis_at))
    return level


def gaussian(stream_key, extent, scale, limit, pieces=(), kind=jnp.bfloat16):
    gain = block_levels(stream_key, extent, pieces, -0.22, 0.18) if pieces else 1.0
    values = jax.random.normal(stream_key, extent, jnp.float32) * scale * gain
    return jnp.minimum(jnp.maximum(values, -limit), limit).astype(kind)


def setup_inputs(seed: int = 0) -> dict:
    splits = jax.random.split(jax.random.key(seed), 6)
    queries = gaussian(splits[0], (SEQUENCE_TOKENS, HEAD_COUNT * DK), 1.0, 6.0, ((0, 128),))
    keys = gaussian(splits[1], (SEQUENCE_TOKENS, HEAD_COUNT * DK), 1.0, 6.0, ((0, 128),))
    values = gaussian(splits[2], (SEQUENCE_TOKENS, HEAD_COUNT * DV), 1.0, 6.0, ((0, 128),))
    grad_out = gaussian(splits[3], (SEQUENCE_TOKENS, HEAD_COUNT * DV), (2 * SEQUENCE_TOKENS ** -0.5), 0.0625, ((0, 128),))
    log_decay = draw_log_decay(jax.random.fold_in(splits[5], 71), 0)
    return dict(queries=queries, keys=keys, values=values, grad_out=grad_out, log_decay=log_decay)


def block_factors(logs):
    cumul = jnp.cumsum(logs, axis=-1)
    ends = cumul[:, -1]
    width = logs.shape[-1]
    lower = jnp.tril(jnp.ones((width, width), dtype=bool))
    spread = cumul[:, :, None] - cumul[:, None, :]
    decay = jnp.where(lower, jnp.exp(jnp.where(lower, spread, 0.0)), 0.0)
    return cumul, ends, decay


def reference(queries, keys, values, grad_out, log_decay):
    count = SEQUENCE_TOKENS // BLOCK
    scale = DK ** -0.5
    query_blocks = queries.reshape(count, BLOCK, HEAD_COUNT, DK)
    key_blocks = keys.reshape(count, BLOCK, HEAD_COUNT, DK)
    value_blocks = values.reshape(count, BLOCK, HEAD_COUNT, DV)
    grad_blocks = grad_out.reshape(count, BLOCK, HEAD_COUNT, DV)
    log_blocks = jnp.transpose(log_decay.reshape(HEAD_COUNT, count, BLOCK), (1, 0, 2))

    def forward_step(state, inputs):
        query_now, key_now, value_now, grad_now, logs = inputs
        query32 = query_now.astype(jnp.float32)
        key32 = key_now.astype(jnp.float32)
        value32 = value_now.astype(jnp.float32)
        grad32 = grad_now.astype(jnp.float32)
        cumul, ends, decay = block_factors(logs)
        scores = jnp.einsum('the,she->hts', grad32, value32)
        weight_grad = lax.optimization_barrier((scores * decay).astype(jnp.bfloat16))
        inner = jnp.einsum('hts,shd->thd', weight_grad.astype(jnp.float32), key32)
        state_low = lax.optimization_barrier(state.astype(jnp.bfloat16))
        outer = jnp.einsum('the,hde->thd', grad32, state_low.astype(jnp.float32))
        outer = outer * jnp.exp(cumul).T[:, :, None]
        result = (scale * (inner + outer)).astype(jnp.bfloat16)
        tail = jnp.exp(ends[:, None] - cumul).T[:, :, None]
        keys_decayed = lax.optimization_barrier((key32 * tail).astype(jnp.bfloat16))
        update = jnp.einsum('shd,she->hde', keys_decayed.astype(jnp.float32), value32)
        state_next = jnp.exp(ends)[:, None, None] * state + update
        return state_next, result

    def reverse_step(state, inputs):
        query_now, key_now, value_now, grad_now, logs = inputs
        query32 = query_now.astype(jnp.float32)
        key32 = key_now.astype(jnp.float32)
        value32 = value_now.astype(jnp.float32)
        grad32 = grad_now.astype(jnp.float32)
        cumul, ends, decay = block_factors(logs)
        scores = jnp.einsum('the,she->hts', grad32, value32)
        weight_grad = lax.optimization_barrier((scores * decay).astype(jnp.bfloat16))
        attend = jnp.einsum('thd,shd->hts', query32, key32)
        weight_value = lax.optimization_barrier((attend * decay).astype(jnp.bfloat16))
        state_low = lax.optimization_barrier(state.astype(jnp.bfloat16)).astype(jnp.float32)
        tail = jnp.exp(ends[:, None] - cumul).T[:, :, None]
        key_grad = jnp.einsum('hts,thd->shd', weight_grad.astype(jnp.float32), query32)
        key_grad = key_grad + tail * jnp.einsum('she,hde->shd', value32, state_low)
        value_grad = jnp.einsum('hts,the->she', weight_value.astype(jnp.float32), grad32)
        value_grad = value_grad + tail * jnp.einsum('shd,hde->she', key32, state_low)
        queries_decayed = lax.optimization_barrier((query32 * jnp.exp(cumul).T[:, :, None]).astype(jnp.bfloat16))
        update = jnp.einsum('thd,the->hde', queries_decayed.astype(jnp.float32), grad32)
        state_next = jnp.exp(ends)[:, None, None] * state + update
        return state_next, ((scale * key_grad).astype(jnp.bfloat16), (scale * value_grad).astype(jnp.bfloat16))

    inputs = (query_blocks, key_blocks, value_blocks, grad_blocks, log_blocks)
    empty = jnp.zeros((HEAD_COUNT, DK, DV), jnp.float32)
    unused, grad_q = lax.scan(forward_step, empty, inputs)
    unused_too, pair = lax.scan(reverse_step, empty, inputs, reverse=True)
    grad_k, grad_v = pair
    return (grad_q.reshape(SEQUENCE_TOKENS, HEAD_COUNT * DK), grad_k.reshape(SEQUENCE_TOKENS, HEAD_COUNT * DK), grad_v.reshape(SEQUENCE_TOKENS, HEAD_COUNT * DV))
```

```python
import jax
import jax.numpy as jnp
from jax import lax
from jax.experimental import pallas as pl
from jax.experimental.pallas import tpu as pltpu
from jax.sharding import Mesh
from jax.sharding import PartitionSpec as P

HEADS = 8
GROUP = 4
D = 256
TOK = 256
CHIPS = ("z", "y", "x")
ALL = ("z", "y", "x", "core")
F32 = jnp.float32
BF16 = jnp.bfloat16
STATE_ROWS = 2 * D + 8


def dot(a, b, ca, cb):
    return lax.dot_general(a, b, (((ca,), (cb,)), ((), ())), preferred_element_type=F32)


def exact_dot(a, b, ca, cb):
    return lax.dot_general(
        a,
        b,
        (((ca,), (cb,)), ((), ())),
        preferred_element_type=F32,
        precision=lax.Precision.HIGHEST,
    )


def lower_mask():
    rows = lax.broadcasted_iota(jnp.int32, (TOK, TOK), 0)
    cols = lax.broadcasted_iota(jnp.int32, (TOK, TOK), 1)
    return cols <= rows


def pick_column(table, head):
    lanes = lax.broadcasted_iota(jnp.int32, table.shape, 1)
    return jnp.sum(jnp.where(lanes == head, table, 0.0), axis=1, keepdims=True)


def states_kernel(grp_ref, log_ref, q_ref, k_ref, v_ref, g_ref, out_ref, col_ref):
    step = pl.program_id(0)

    @pl.when(step == 0)
    def _():
        tri = jnp.where(lower_mask(), 1.0, 0.0)
        col_ref[...] = exact_dot(tri, log_ref[...], 1, 1)

    head = grp_ref[0] * GROUP + step
    cumul = pick_column(col_ref[...], head)
    end = cumul[TOK - 1 : TOK, :]
    keys = (k_ref[...].astype(F32) * jnp.exp(end - cumul)).astype(BF16)
    queries = (q_ref[...].astype(F32) * jnp.exp(cumul)).astype(BF16)
    out_ref[0, 0:D, :] = dot(keys, v_ref[...], 0, 0)
    out_ref[0, D : 2 * D, :] = dot(queries, g_ref[...], 0, 0)
    out_ref[0, 2 * D : STATE_ROWS, :] = jnp.broadcast_to(jnp.exp(end), (8, D))


def head_spec():
    return pl.BlockSpec((TOK, D), lambda i, grp: (0, grp[0] * GROUP + i))


def whole(shape):
    return pl.BlockSpec(shape, lambda i, grp: (0,) * len(shape))


def device_states(grp, log_decay, q, k, v, g):
    return pl.pallas_call(
        states_kernel,
        out_shape=jax.ShapeDtypeStruct((GROUP, STATE_ROWS, D), F32),
        grid_spec=pltpu.PrefetchScalarGridSpec(
            num_scalar_prefetch=1,
            grid=(GROUP,),
            in_specs=[whole((HEADS, TOK))] + [head_spec()] * 4,
            out_specs=pl.BlockSpec((1, STATE_ROWS, D), lambda i, grp: (i, 0, 0)),
            scratch_shapes=[pltpu.VMEM((TOK, HEADS), F32)],
        ),
        name="device_states",
    )(grp, log_decay, q, k, v, g)


def combine_kernel(core_ref, own_ref, other_ref, out_ref):
    first = core_ref[0] == 0
    own_decay = own_ref[0, 2 * D : 2 * D + 1, 0:128]
    other_decay = other_ref[0, 2 * D : 2 * D + 1, 0:128]
    one = jnp.ones_like(own_decay)
    fwd_own = jnp.where(first, other_decay, one)
    fwd_other = jnp.where(first, one, own_decay)
    rev_own = jnp.where(first, one, other_decay)
    rev_other = jnp.where(first, own_decay, one)
    for half in range(2):
        lanes = slice(128 * half, 128 * half + 128)
        fwd = fwd_own * own_ref[0, 0:D, lanes] + fwd_other * other_ref[0, 0:D, lanes]
        rev = rev_own * own_ref[0, D : 2 * D, lanes] + rev_other * other_ref[0, D : 2 * D, lanes]
        out_ref[:, 16 * half : 16 * half + 16, :] = fwd.reshape(16, 16, 128)
        out_ref[:, 32 + 16 * half : 48 + 16 * half, :] = rev.reshape(16, 16, 128)
    out_ref[:, 64:72, :] = jnp.broadcast_to((own_decay * other_decay)[None], (16, 8, 128))


def combine(core, own, other):
    state = pl.BlockSpec((1, STATE_ROWS, D), lambda i, core: (i, 0, 0))
    return pl.pallas_call(
        combine_kernel,
        out_shape=jax.ShapeDtypeStruct((64, 72, 128), F32),
        grid_spec=pltpu.PrefetchScalarGridSpec(
            num_scalar_prefetch=1,
            grid=(GROUP,),
            in_specs=[state, state],
            out_specs=pl.BlockSpec((16, 72, 128), lambda i, core: (i, 0, 0)),
        ),
        name="combine_cores",
    )(core, own, other)


def scan_kernel(in_ref, out_ref):
    def fwd_step(chip, carry):
        out_ref[chip, 0:32, :] = carry
        decay = in_ref[chip, 64:65, :]
        return decay * carry + in_ref[chip, 0:32, :]

    def rev_step(index, carry):
        chip = 63 - index
        out_ref[chip, 32:64, :] = carry
        decay = in_ref[chip, 64:65, :]
        return decay * carry + in_ref[chip, 32:64, :]

    def both(index, carry):
        return fwd_step(index, carry[0]), rev_step(index, carry[1])

    zero = jnp.zeros((32, 128), F32)
    lax.fori_loop(0, 64, both, (zero, zero), unroll=8)


def scan_chips(received):
    return pl.pallas_call(
        scan_kernel,
        out_shape=jax.ShapeDtypeStruct((64, 64, 128), F32),
        in_specs=[pl.BlockSpec(memory_space=pltpu.VMEM)],
        out_specs=pl.BlockSpec(memory_space=pltpu.VMEM),
        name="scan_chips",
    )(received)


def middle_kernel(core_ref, back_ref, own_ref, other_ref, keep_ref, send_ref):
    first = core_ref[0] == 0
    own_decay = own_ref[0, 2 * D : 2 * D + 1, 0:128]
    other_decay = other_ref[0, 2 * D : 2 * D + 1, 0:128]
    fwd_decay = jnp.where(first, own_decay, other_decay)
    rev_decay = jnp.where(first, other_decay, own_decay)
    for half in range(2):
        lanes = slice(128 * half, 128 * half + 128)
        fwd_enter = back_ref[:, 16 * half : 16 * half + 16, :].reshape(D, 128)
        rev_enter = back_ref[:, 32 + 16 * half : 48 + 16 * half, :].reshape(D, 128)
        fwd_part = jnp.where(first, own_ref[0, 0:D, lanes], other_ref[0, 0:D, lanes])
        rev_part = jnp.where(first, other_ref[0, D : 2 * D, lanes], own_ref[0, D : 2 * D, lanes])
        fwd_mid = fwd_decay * fwd_enter + fwd_part
        rev_mid = rev_decay * rev_enter + rev_part
        keep_ref[0, 0:D, lanes] = jnp.where(first, fwd_enter, fwd_mid)
        keep_ref[0, D : 2 * D, lanes] = jnp.where(first, rev_mid, rev_enter)
        send_ref[0, 0:D, lanes] = jnp.where(first, fwd_mid, fwd_enter)
        send_ref[0, D : 2 * D, lanes] = jnp.where(first, rev_enter, rev_mid)


def middle(core, back, own, other):
    state = pl.BlockSpec((1, STATE_ROWS, D), lambda i, core: (i, 0, 0))
    pair = pl.BlockSpec((1, 2 * D, D), lambda i, core: (i, 0, 0))
    return pl.pallas_call(
        middle_kernel,
        out_shape=[jax.ShapeDtypeStruct((GROUP, 2 * D, D), F32)] * 2,
        grid_spec=pltpu.PrefetchScalarGridSpec(
            num_scalar_prefetch=1,
            grid=(GROUP,),
            in_specs=[pl.BlockSpec((16, 64, 128), lambda i, core: (i, 0, 0)), state, state],
            out_specs=[pair, pair],
        ),
        name="middle_states",
    )(core, back, own, other)


def grads_kernel(grp_ref, log_ref, q_ref, k_ref, v_ref, g_ref, st_ref, *rest):
    gq_ref, gk_ref, gv_ref, col_ref, row_ref = rest[-5:]
    step = pl.program_id(0)

    @pl.when(step == 0)
    def _():
        tri = jnp.where(lower_mask(), 1.0, 0.0)
        col_ref[...] = exact_dot(tri, log_ref[...], 1, 1)
        row_ref[...] = exact_dot(log_ref[...], tri, 1, 1)

    head = grp_ref[0] * GROUP + step
    scale = D ** (-0.5)
    col = pick_column(col_ref[...], head)
    row = row_ref[pl.ds(head, 1), :]
    lower = lower_mask()
    decay = jnp.where(lower, jnp.exp(jnp.where(lower, col - row, 0.0)), 0.0)
    head_factor = jnp.exp(col)
    tail_factor = jnp.exp(col[TOK - 1 : TOK, :] - col)
    q, k, v, g = q_ref[...], k_ref[...], v_ref[...], g_ref[...]
    fwd = st_ref[0, 0:D, :].astype(BF16)
    rev = st_ref[0, D : 2 * D, :].astype(BF16)
    weight_grad = (dot(g, v, 1, 1) * decay).astype(BF16)
    weight_value = (dot(q, k, 1, 1) * decay).astype(BF16)
    gq = dot(weight_grad, k, 1, 0) + head_factor * dot(g, fwd, 1, 1)
    gq_ref[...] = (scale * gq).astype(BF16)
    gk = dot(weight_grad, q, 0, 0) + tail_factor * dot(v, rev, 1, 1)
    gk_ref[...] = (scale * gk).astype(BF16)
    gv = dot(weight_value, g, 0, 0) + tail_factor * dot(k, rev, 1, 0)
    gv_ref[...] = (scale * gv).astype(BF16)


def gradients(grp, log_decay, q, k, v, g, states, started=()):
    shape = jax.ShapeDtypeStruct((TOK, HEADS * D), BF16)
    count = len(started)
    return pl.pallas_call(
        grads_kernel,
        out_shape=[shape] * 3,
        grid_spec=pltpu.PrefetchScalarGridSpec(
            num_scalar_prefetch=1,
            grid=(GROUP,),
            in_specs=[whole((HEADS, TOK))]
            + [head_spec()] * 4
            + [pl.BlockSpec((1, 2 * D, D), lambda i, grp: (i, 0, 0))]
            + [pl.BlockSpec(memory_space=pl.ANY)] * count,
            out_specs=[head_spec()] * 3,
            scratch_shapes=[pltpu.VMEM((TOK, HEADS), F32), pltpu.VMEM((HEADS, TOK), F32)],
        ),
        input_output_aliases={7 + n: n for n in range(count)},
        name="gradients",
    )(grp, log_decay, q, k, v, g, states, *started)


def body(queries, keys, values, grad_out, log_decay):
    core = lax.axis_index("core").astype(jnp.int32).reshape(1)
    other_core = 1 - core
    swap = [(0, 1), (1, 0)]
    tokens = (log_decay, queries, keys, values, grad_out)
    for_other = device_states(other_core, *tokens)
    from_other = lax.ppermute(for_other, "core", swap)
    own = device_states(core, *tokens)
    payload = combine(core, own, from_other)
    received = lax.all_to_all(payload.reshape(64 * 72, 128), CHIPS, 0, 0, tiled=True)
    prefixes = scan_chips(received.reshape(64, 72, 128))
    back = lax.all_to_all(prefixes.reshape(64 * 64, 128), CHIPS, 0, 0, tiled=True)
    keep, send = middle(core, back.reshape(64, 64, 128), own, from_other)
    arrived = lax.ppermute(send, "core", swap)
    started = gradients(core, *tokens, keep)
    return tuple(gradients(other_core, *tokens, arrived, started))


def solution(mesh):
    torus = Mesh(mesh.devices.reshape(4, 4, 4, 2), ALL)
    rows = P(ALL, None)
    return jax.shard_map(
        body,
        mesh=torus,
        in_specs=(rows, rows, rows, rows, P(None, ALL)),
        out_specs=(rows, rows, rows),
        check_vma=False,
    )
```

```python
import jax
import jax.numpy as jnp
from jax import lax
from jax.experimental import pallas as pl
from jax.experimental.pallas import tpu as pltpu
from jax.sharding import Mesh
from jax.sharding import PartitionSpec as P

HEADS = 8
GROUP = 4
D = 256
TOK = 256
CHIPS = ("z", "y", "x")
ALL = ("z", "y", "x", "core")
F32 = jnp.float32
BF16 = jnp.bfloat16
STATE_ROWS = 2 * D + 8
VMEM_LIMIT = 12 * 1024 * 1024


def dot(a, b, ca, cb):
    return lax.dot_general(a, b, (((ca,), (cb,)), ((), ())), preferred_element_type=F32)


def exact_dot(a, b, ca, cb):
    return lax.dot_general(
        a,
        b,
        (((ca,), (cb,)), ((), ())),
        preferred_element_type=F32,
        precision=lax.Precision.HIGHEST,
    )


def lower_mask():
    rows = lax.broadcasted_iota(jnp.int32, (TOK, TOK), 0)
    cols = lax.broadcasted_iota(jnp.int32, (TOK, TOK), 1)
    return cols <= rows


def pick_column(table, head):
    lanes = lax.broadcasted_iota(jnp.int32, table.shape, 1)
    return jnp.sum(jnp.where(lanes == head, table, 0.0), axis=1, keepdims=True)


def states_kernel(grp_ref, log_ref, q_ref, k_ref, v_ref, g_ref, out_ref, col_ref):
    step = pl.program_id(0)

    @pl.when(step == 0)
    def _():
        tri = jnp.where(lower_mask(), 1.0, 0.0)
        col_ref[...] = exact_dot(tri, log_ref[...], 1, 1)

    head = grp_ref[0] * GROUP + step
    cumul = pick_column(col_ref[...], head)
    end = cumul[TOK - 1 : TOK, :]
    keys = (k_ref[...].astype(F32) * jnp.exp(end - cumul)).astype(BF16)
    queries = (q_ref[...].astype(F32) * jnp.exp(cumul)).astype(BF16)
    out_ref[0, 0:D, :] = dot(keys, v_ref[...], 0, 0)
    out_ref[0, D : 2 * D, :] = dot(queries, g_ref[...], 0, 0)
    out_ref[0, 2 * D : STATE_ROWS, :] = jnp.broadcast_to(jnp.exp(end), (8, D))


def head_spec():
    return pl.BlockSpec((TOK, D), lambda i, grp: (0, grp[0] * GROUP + i))


def whole(shape):
    return pl.BlockSpec(shape, lambda i, grp: (0,) * len(shape))


def device_states(grp, log_decay, q, k, v, g):
    return pl.pallas_call(
        states_kernel,
        out_shape=jax.ShapeDtypeStruct((GROUP, STATE_ROWS, D), F32),
        grid_spec=pltpu.PrefetchScalarGridSpec(
            num_scalar_prefetch=1,
            grid=(GROUP,),
            in_specs=[whole((HEADS, TOK))] + [head_spec()] * 4,
            out_specs=pl.BlockSpec((1, STATE_ROWS, D), lambda i, grp: (i, 0, 0)),
            scratch_shapes=[pltpu.VMEM((TOK, HEADS), F32)],
        ),
        compiler_params=pltpu.CompilerParams(vmem_limit_bytes=VMEM_LIMIT),
        name="device_states",
    )(grp, log_decay, q, k, v, g)


def combine_kernel(core_ref, own_ref, other_ref, out_ref):
    first = core_ref[0] == 0
    own_decay = own_ref[0, 2 * D : 2 * D + 1, 0:128]
    other_decay = other_ref[0, 2 * D : 2 * D + 1, 0:128]
    one = jnp.ones_like(own_decay)
    fwd_own = jnp.where(first, other_decay, one)
    fwd_other = jnp.where(first, one, own_decay)
    rev_own = jnp.where(first, one, other_decay)
    rev_other = jnp.where(first, own_decay, one)
    for half in range(2):
        lanes = slice(128 * half, 128 * half + 128)
        fwd = fwd_own * own_ref[0, 0:D, lanes] + fwd_other * other_ref[0, 0:D, lanes]
        rev = rev_own * own_ref[0, D : 2 * D, lanes] + rev_other * other_ref[0, D : 2 * D, lanes]
        out_ref[:, 16 * half : 16 * half + 16, :] = fwd.reshape(16, 16, 128)
        out_ref[:, 32 + 16 * half : 48 + 16 * half, :] = rev.reshape(16, 16, 128)
    out_ref[:, 64:72, :] = jnp.broadcast_to((own_decay * other_decay)[None], (16, 8, 128))


def combine(core, own, other):
    state = pl.BlockSpec((1, STATE_ROWS, D), lambda i, core: (i, 0, 0))
    return pl.pallas_call(
        combine_kernel,
        out_shape=jax.ShapeDtypeStruct((64, 72, 128), F32),
        grid_spec=pltpu.PrefetchScalarGridSpec(
            num_scalar_prefetch=1,
            grid=(GROUP,),
            in_specs=[state, state],
            out_specs=pl.BlockSpec((16, 72, 128), lambda i, core: (i, 0, 0)),
        ),
        compiler_params=pltpu.CompilerParams(vmem_limit_bytes=VMEM_LIMIT),
        name="combine_cores",
    )(core, own, other)


def scan_kernel(in_ref, out_ref):
    def fwd_step(chip, carry):
        out_ref[chip, 0:32, :] = carry
        decay = in_ref[chip, 64:65, :]
        return decay * carry + in_ref[chip, 0:32, :]

    def rev_step(index, carry):
        chip = 63 - index
        out_ref[chip, 32:64, :] = carry
        decay = in_ref[chip, 64:65, :]
        return decay * carry + in_ref[chip, 32:64, :]

    def both(index, carry):
        return fwd_step(index, carry[0]), rev_step(index, carry[1])

    zero = jnp.zeros((32, 128), F32)
    lax.fori_loop(0, 64, both, (zero, zero), unroll=8)


def scan_chips(received):
    return pl.pallas_call(
        scan_kernel,
        out_shape=jax.ShapeDtypeStruct((64, 64, 128), F32),
        in_specs=[pl.BlockSpec(memory_space=pltpu.VMEM)],
        out_specs=pl.BlockSpec(memory_space=pltpu.VMEM),
        compiler_params=pltpu.CompilerParams(vmem_limit_bytes=VMEM_LIMIT),
        name="scan_chips",
    )(received)


def middle_kernel(core_ref, back_ref, own_ref, other_ref, keep_ref, send_ref):
    first = core_ref[0] == 0
    own_decay = own_ref[0, 2 * D : 2 * D + 1, 0:128]
    other_decay = other_ref[0, 2 * D : 2 * D + 1, 0:128]
    fwd_decay = jnp.where(first, own_decay, other_decay)
    rev_decay = jnp.where(first, other_decay, own_decay)
    for half in range(2):
        lanes = slice(128 * half, 128 * half + 128)
        fwd_enter = back_ref[:, 16 * half : 16 * half + 16, :].reshape(D, 128)
        rev_enter = back_ref[:, 32 + 16 * half : 48 + 16 * half, :].reshape(D, 128)
        fwd_part = jnp.where(first, own_ref[0, 0:D, lanes], other_ref[0, 0:D, lanes])
        rev_part = jnp.where(first, other_ref[0, D : 2 * D, lanes], own_ref[0, D : 2 * D, lanes])
        fwd_mid = fwd_decay * fwd_enter + fwd_part
        rev_mid = rev_decay * rev_enter + rev_part
        keep_ref[0, 0:D, lanes] = jnp.where(first, fwd_enter, fwd_mid)
        keep_ref[0, D : 2 * D, lanes] = jnp.where(first, rev_mid, rev_enter)
        send_ref[0, 0:D, lanes] = jnp.where(first, fwd_mid, fwd_enter)
        send_ref[0, D : 2 * D, lanes] = jnp.where(first, rev_enter, rev_mid)


def middle(core, back, own, other):
    state = pl.BlockSpec((1, STATE_ROWS, D), lambda i, core: (i, 0, 0))
    pair = pl.BlockSpec((1, 2 * D, D), lambda i, core: (i, 0, 0))
    return pl.pallas_call(
        middle_kernel,
        out_shape=[jax.ShapeDtypeStruct((GROUP, 2 * D, D), F32)] * 2,
        grid_spec=pltpu.PrefetchScalarGridSpec(
            num_scalar_prefetch=1,
            grid=(GROUP,),
            in_specs=[pl.BlockSpec((16, 64, 128), lambda i, core: (i, 0, 0)), state, state],
            out_specs=[pair, pair],
        ),
        compiler_params=pltpu.CompilerParams(vmem_limit_bytes=VMEM_LIMIT),
        name="middle_states",
    )(core, back, own, other)


def grads_kernel(grp_ref, log_ref, q_ref, k_ref, v_ref, g_ref, st_ref, *rest):
    gq_ref, gk_ref, gv_ref, col_ref, row_ref = rest[-5:]
    step = pl.program_id(0)

    @pl.when(step == 0)
    def _():
        tri = jnp.where(lower_mask(), 1.0, 0.0)
        col_ref[...] = exact_dot(tri, log_ref[...], 1, 1)
        row_ref[...] = exact_dot(log_ref[...], tri, 1, 1)

    head = grp_ref[0] * GROUP + step
    scale = D ** (-0.5)
    col = pick_column(col_ref[...], head)
    row = row_ref[pl.ds(head, 1), :]
    lower = lower_mask()
    decay = jnp.where(lower, jnp.exp(jnp.where(lower, col - row, 0.0)), 0.0)
    head_factor = jnp.exp(col)
    tail_factor = jnp.exp(col[TOK - 1 : TOK, :] - col)
    q, k, v, g = q_ref[...], k_ref[...], v_ref[...], g_ref[...]
    fwd = st_ref[0, 0:D, :].astype(BF16)
    rev = st_ref[0, D : 2 * D, :].astype(BF16)
    weight_grad = (dot(g, v, 1, 1) * decay).astype(BF16)
    weight_value = (dot(q, k, 1, 1) * decay).astype(BF16)
    gq = dot(weight_grad, k, 1, 0) + head_factor * dot(g, fwd, 1, 1)
    gq_ref[...] = (scale * gq).astype(BF16)
    gk = dot(weight_grad, q, 0, 0) + tail_factor * dot(v, rev, 1, 1)
    gk_ref[...] = (scale * gk).astype(BF16)
    gv = dot(weight_value, g, 0, 0) + tail_factor * dot(k, rev, 1, 0)
    gv_ref[...] = (scale * gv).astype(BF16)


def gradients(grp, log_decay, q, k, v, g, states, started=()):
    shape = jax.ShapeDtypeStruct((TOK, HEADS * D), BF16)
    count = len(started)
    return pl.pallas_call(
        grads_kernel,
        out_shape=[shape] * 3,
        grid_spec=pltpu.PrefetchScalarGridSpec(
            num_scalar_prefetch=1,
            grid=(GROUP,),
            in_specs=[whole((HEADS, TOK))]
            + [head_spec()] * 4
            + [pl.BlockSpec((1, 2 * D, D), lambda i, grp: (i, 0, 0))]
            + [pl.BlockSpec(memory_space=pl.ANY)] * count,
            out_specs=[head_spec()] * 3,
            scratch_shapes=[pltpu.VMEM((TOK, HEADS), F32), pltpu.VMEM((HEADS, TOK), F32)],
        ),
        input_output_aliases={7 + n: n for n in range(count)},
        compiler_params=pltpu.CompilerParams(vmem_limit_bytes=VMEM_LIMIT),
        name="gradients",
    )(grp, log_decay, q, k, v, g, states, *started)


def body(queries, keys, values, grad_out, log_decay):
    core = lax.axis_index("core").astype(jnp.int32).reshape(1)
    other_core = 1 - core
    swap = [(0, 1), (1, 0)]
    tokens = (log_decay, queries, keys, values, grad_out)
    for_other = device_states(other_core, *tokens)
    from_other = lax.ppermute(for_other, "core", swap)
    own = device_states(core, *tokens)
    payload = combine(core, own, from_other)
    received = lax.all_to_all(payload.reshape(64 * 72, 128), CHIPS, 0, 0, tiled=True)
    prefixes = scan_chips(received.reshape(64, 72, 128))
    back = lax.all_to_all(prefixes.reshape(64 * 64, 128), CHIPS, 0, 0, tiled=True)
    keep, send = middle(core, back.reshape(64, 64, 128), own, from_other)
    arrived = lax.ppermute(send, "core", swap)
    started = gradients(core, *tokens, keep)
    return tuple(gradients(other_core, *tokens, arrived, started))


def solution(mesh):
    torus = Mesh(mesh.devices.reshape(4, 4, 4, 2), ALL)
    rows = P(ALL, None)
    return jax.shard_map(
        body,
        mesh=torus,
        in_specs=(rows, rows, rows, rows, P(None, ALL)),
        out_specs=(rows, rows, rows),
        check_vma=False,
    )
```

```python
import functools

import jax
import jax.numpy as jnp
from jax import lax
from jax.experimental import pallas as pl
from jax.experimental.pallas import tpu as pltpu
from jax.sharding import Mesh
from jax.sharding import PartitionSpec as P

HEADS = 8
GROUP = 4
PAIR = 2
D = 256
TOK = 256
RING = 4
XROWS = D // RING
YROWS = XROWS // RING
ALL = ("z", "y", "x", "core")
F32 = jnp.float32
BF16 = jnp.bfloat16
STATE_ROWS = 2 * D + 8
SCALE = D ** (-0.5)
VMEM_LIMIT = 10 * 1024 * 1024
CORE, Z, Y, X = range(4)


def dot(a, b, ca, cb):
    return lax.dot_general(a, b, (((ca,), (cb,)), ((), ())), preferred_element_type=F32)


def exact_dot(a, b, ca, cb):
    return lax.dot_general(
        a,
        b,
        (((ca,), (cb,)), ((), ())),
        preferred_element_type=F32,
        precision=lax.Precision.HIGHEST,
    )


def lower_mask():
    rows = lax.broadcasted_iota(jnp.int32, (TOK, TOK), 0)
    cols = lax.broadcasted_iota(jnp.int32, (TOK, TOK), 1)
    return cols <= rows


def pick_column(table, column):
    lanes = lax.broadcasted_iota(jnp.int32, table.shape, 1)
    return jnp.sum(jnp.where(lanes == column, table, 0.0), axis=1, keepdims=True)


def params(limit=VMEM_LIMIT):
    return pltpu.CompilerParams(vmem_limit_bytes=limit)


def shaped(*shape):
    return jax.ShapeDtypeStruct(shape, F32)


def vmem_call(kernel, name, out_shape, ids, operands, scratch=()):
    vmem = pl.BlockSpec(memory_space=pltpu.VMEM)
    return pl.pallas_call(
        kernel,
        out_shape=out_shape,
        in_specs=[pl.BlockSpec(memory_space=pltpu.SMEM)] + [vmem] * len(operands),
        out_specs=jax.tree.map(lambda _: vmem, out_shape),
        scratch_shapes=list(scratch),
        compiler_params=params(),
        name=name,
    )(ids, *operands)


def first_head(ids, own, base):
    group = ids[CORE] if own else 1 - ids[CORE]
    return group * GROUP + base


def write_state(out_ref, slot, factors, head, q, k, v, g):
    rising = pick_column(factors, head)
    falling = pick_column(factors, head + HEADS)
    keys = (k.astype(F32) * falling).astype(BF16)
    queries = (q.astype(F32) * rising).astype(BF16)
    out_ref[slot, 0:D, :] = dot(keys, v, 0, 0)
    out_ref[slot, D : 2 * D, :] = dot(queries, g, 0, 0)
    out_ref[slot, 2 * D : STATE_ROWS, :] = jnp.broadcast_to(rising[TOK - 1 :, :], (8, D))


def load_kernel(ids, log_ref, q_hbm, k_hbm, v_hbm, g_hbm, out_ref, fac_ref, *rest):
    sources = (q_hbm, k_hbm, v_hbm, g_hbm)
    targets = rest[:4]
    sems = rest[4]
    other = 1 - ids[CORE]
    copies = []
    for order in range(HEADS):
        group = other if order < GROUP else 1 - other
        start = pl.multiple_of((group * GROUP + order % GROUP) * D, D)
        lanes = pl.ds(start, D)
        row = []
        for index in range(4):
            copy = pltpu.make_async_copy(
                sources[index].at[:, lanes],
                targets[index].at[:, lanes],
                sems.at[order * 4 + index],
            )
            copy.start()
            row.append(copy)
        copies.append(row)
    tri = jnp.where(lower_mask(), 1.0, 0.0)
    cumul = exact_dot(tri, log_ref[...], 1, 1)
    fac_ref[:, 0:HEADS] = jnp.exp(cumul)
    fac_ref[:, HEADS : 2 * HEADS] = jnp.exp(cumul[TOK - 1 :, :] - cumul)
    factors = fac_ref[...]
    for order in range(PAIR):
        for copy in copies[order]:
            copy.wait()
        head = other * GROUP + order
        lanes = pl.ds(pl.multiple_of(head * D, D), D)
        parts = [target[:, lanes] for target in targets]
        write_state(out_ref, order, factors, head, *parts)
    for order in range(PAIR, HEADS):
        for copy in copies[order]:
            copy.wait()


def load_and_start(ids, log_decay, *tokens):
    array = jax.ShapeDtypeStruct((TOK, HEADS * D), BF16)
    vmem = pl.BlockSpec(memory_space=pltpu.VMEM)
    tokens = [pltpu.with_memory_space_constraint(t, pltpu.HBM) for t in tokens]
    return pl.pallas_call(
        load_kernel,
        out_shape=[shaped(PAIR, STATE_ROWS, D), shaped(TOK, 2 * HEADS)] + [array] * 4,
        in_specs=[pl.BlockSpec(memory_space=pltpu.SMEM), vmem]
        + [pl.BlockSpec(memory_space=pl.ANY)] * 4,
        out_specs=[vmem] * 6,
        scratch_shapes=[pltpu.SemaphoreType.DMA((4 * HEADS,))],
        compiler_params=params(),
        name="load_and_start",
    )(ids, log_decay, *tokens)


def states_kernel(own, base, ids, fac_ref, q_ref, k_ref, v_ref, g_ref, out_ref):
    head = first_head(ids, own, base) + pl.program_id(0)
    write_state(out_ref, 0, fac_ref[...], head, q_ref[...], k_ref[...], v_ref[...], g_ref[...])


def head_spec(own, base):
    return pl.BlockSpec((TOK, D), lambda i, ids: (0, first_head(ids, own, base) + i))


def whole(shape):
    return pl.BlockSpec(shape, lambda i, ids: (0,) * len(shape))


def device_states(ids, own, base, factors, *tokens):
    return pl.pallas_call(
        functools.partial(states_kernel, own, base),
        out_shape=shaped(PAIR, STATE_ROWS, D),
        grid_spec=pltpu.PrefetchScalarGridSpec(
            num_scalar_prefetch=1,
            grid=(PAIR,),
            in_specs=[whole((TOK, 2 * HEADS))] + [head_spec(own, base)] * 4,
            out_specs=pl.BlockSpec((1, STATE_ROWS, D), lambda i, ids: (i, 0, 0)),
        ),
        compiler_params=params(),
        name="device_states",
    )(ids, factors, *tokens)


def rows_of(index, size):
    return pl.ds(pl.multiple_of(index * size, size), size)


def combine_kernel(ids, own_ref, other_ref, *outs):
    first = ids[CORE] == 0
    for head in range(PAIR):
        own_decay = own_ref[head, 2 * D : 2 * D + 1, :]
        other_decay = other_ref[head, 2 * D : 2 * D + 1, :]
        one = jnp.ones_like(own_decay)
        fwd_own = jnp.where(first, other_decay, one)
        fwd_other = jnp.where(first, one, own_decay)
        rev_own = jnp.where(first, one, other_decay)
        rev_other = jnp.where(first, own_decay, one)
        both = jnp.broadcast_to(own_decay * other_decay, (8, D))
        for shift in range(RING):
            place = lax.rem(ids[X] + shift, RING)
            low = rows_of(place, XROWS)
            high = rows_of(place + RING, XROWS)
            out_ref = outs[shift]
            out_ref[head, 0:XROWS, :] = (
                fwd_own * own_ref[head, low, :] + fwd_other * other_ref[head, low, :]
            )
            out_ref[head, XROWS : 2 * XROWS, :] = (
                rev_own * own_ref[head, high, :] + rev_other * other_ref[head, high, :]
            )
            out_ref[head, 2 * XROWS :, :] = both


def ordered(position, refs):
    return [refs[(j - position) % RING] for j in range(RING)]


def on_each(index, visit):
    for position in range(RING):
        pl.when(index == position)(functools.partial(visit, position))


def totals(members, head, size):
    fwd = members[0][head, 0:size, :]
    rev = members[RING - 1][head, size : 2 * size, :]
    decays = [ref[head, 2 * size : 2 * size + 1, :] for ref in members]
    product = decays[0]
    for j in range(1, RING):
        fwd = decays[j] * fwd + members[j][head, 0:size, :]
        back = RING - 1 - j
        rev = decays[back] * rev + members[back][head, size : 2 * size, :]
        product = product * decays[j]
    return fwd, rev, product


def row_kernel(ids, *refs):
    received, outs, sum_ref = refs[:RING], refs[RING : 2 * RING], refs[2 * RING]

    def visit(position):
        members = ordered(position, received)
        for head in range(PAIR):
            fwd, rev, product = totals(members, head, XROWS)
            sum_ref[head, 0:XROWS, :] = fwd
            sum_ref[head, XROWS : 2 * XROWS, :] = rev
            sum_ref[head, 2 * XROWS :, :] = jnp.broadcast_to(product, (8, D))

    on_each(ids[X], visit)
    for shift in range(RING):
        place = lax.rem(ids[Y] + shift, RING)
        for head in range(PAIR):
            outs[shift][head, 0:YROWS, :] = sum_ref[head, rows_of(place, YROWS), :]
            outs[shift][head, YROWS : 2 * YROWS, :] = sum_ref[
                head, rows_of(place + RING, YROWS), :
            ]
            outs[shift][head, 2 * YROWS :, :] = sum_ref[head, 2 * XROWS :, :]


def plane_kernel(ids, *refs):
    received, outs = refs[:RING], refs[RING:]

    def visit(position):
        members = ordered(position, received)
        for head in range(PAIR):
            fwd, rev, product = totals(members, head, YROWS)
            for shift in range(1, RING):
                out_ref = outs[shift - 1]
                later = ids[Z] + shift < RING
                out_ref[head, 0:YROWS, :] = jnp.where(later, fwd, rev)
                out_ref[head, YROWS:, :] = jnp.broadcast_to(product, (8, D))

    on_each(ids[Y], visit)


def prefixes(members, head, size, fwd, rev, store):
    decays = [ref[head, 2 * size : 2 * size + 1, :] for ref in members]
    for j in range(RING):
        store(j, 0, fwd)
        if j < RING - 1:
            fwd = decays[j] * fwd + members[j][head, 0:size, :]
    for j in reversed(range(RING)):
        store(j, 1, rev)
        if j > 0:
            rev = decays[j] * rev + members[j][head, size : 2 * size, :]


def outer_kernel(ids, *refs):
    planes, received = refs[: RING - 1], refs[RING - 1 : 2 * RING - 1]
    outs, sum_ref = refs[2 * RING - 1 : 3 * RING - 1], refs[3 * RING - 1]

    def visit_plane(position):
        def take(j, head):
            ref = planes[(j - position) % RING - 1]
            return ref[head, 0:YROWS, :], ref[head, YROWS : YROWS + 1, :]

        for head in range(PAIR):
            fwd = rev = jnp.zeros((YROWS, D), F32)
            for j in range(position):
                part, decay = take(j, head)
                fwd = part if j == 0 else decay * fwd + part
            for j in reversed(range(position + 1, RING)):
                part, decay = take(j, head)
                rev = part if j == RING - 1 else decay * rev + part
            sum_ref[head, 0:YROWS, :] = fwd
            sum_ref[head, YROWS : 2 * YROWS, :] = rev

    def visit_row(position):
        members = ordered(position, received)
        for head in range(PAIR):

            def store(j, kind, value):
                outs[(j - position) % RING][head, kind * YROWS : (kind + 1) * YROWS, :] = value

            fwd = sum_ref[head, 0:YROWS, :]
            rev = sum_ref[head, YROWS : 2 * YROWS, :]
            prefixes(members, head, YROWS, fwd, rev, store)

    on_each(ids[Z], visit_plane)
    on_each(ids[Y], visit_row)


def chip_kernel(ids, *refs):
    returned, received = refs[:RING], refs[RING : 2 * RING]
    outs, sum_ref = refs[2 * RING : 3 * RING], refs[3 * RING]
    for shift in range(RING):
        place = lax.rem(ids[Y] + shift, RING)
        for head in range(PAIR):
            sum_ref[head, rows_of(place, YROWS), :] = returned[shift][head, 0:YROWS, :]
            sum_ref[head, rows_of(place + RING, YROWS), :] = returned[shift][head, YROWS:, :]

    def visit(position):
        members = ordered(position, received)
        for head in range(PAIR):

            def store(j, kind, value):
                outs[(j - position) % RING][head, kind * XROWS : (kind + 1) * XROWS, :] = value

            fwd = sum_ref[head, 0:XROWS, :]
            rev = sum_ref[head, XROWS : 2 * XROWS, :]
            prefixes(members, head, XROWS, fwd, rev, store)

    on_each(ids[X], visit)


def middle_kernel(own, ids, *refs):
    returned, own_ref, other_ref, out_ref = refs[:RING], refs[RING], refs[RING + 1], refs[RING + 2]
    first = ids[CORE] == 0
    take_first = first if own else ids[CORE] == 1
    for head in range(PAIR):
        own_decay = own_ref[head, 2 * D : 2 * D + 1, :]
        other_decay = other_ref[head, 2 * D : 2 * D + 1, :]
        fwd_decay = jnp.where(first, own_decay, other_decay)
        rev_decay = jnp.where(first, other_decay, own_decay)
        for shift in range(RING):
            place = lax.rem(ids[X] + shift, RING)
            low = rows_of(place, XROWS)
            high = rows_of(place + RING, XROWS)
            fwd_enter = returned[shift][head, 0:XROWS, :]
            rev_enter = returned[shift][head, XROWS : 2 * XROWS, :]
            fwd_part = jnp.where(first, own_ref[head, low, :], other_ref[head, low, :])
            rev_part = jnp.where(first, other_ref[head, high, :], own_ref[head, high, :])
            fwd_mid = fwd_decay * fwd_enter + fwd_part
            rev_mid = rev_decay * rev_enter + rev_part
            out_ref[head, low, :] = jnp.where(take_first, fwd_enter, fwd_mid)
            out_ref[head, high, :] = jnp.where(take_first, rev_mid, rev_enter)


def inner_kernel(own, base, ids, log_ref, q_ref, k_ref, v_ref, g_ref, *rest):
    iq_ref, ik_ref, iv_ref, col_ref, row_ref = rest
    step = pl.program_id(0)

    @pl.when(step == 0)
    def _():
        tri = jnp.where(lower_mask(), 1.0, 0.0)
        col_ref[...] = exact_dot(tri, log_ref[...], 1, 1)
        row_ref[...] = exact_dot(log_ref[...], tri, 1, 1)

    head = first_head(ids, own, base) + step
    col = pick_column(col_ref[...], head)
    row = row_ref[pl.ds(head, 1), :]
    lower = lower_mask()
    decay = jnp.where(lower, jnp.exp(jnp.where(lower, col - row, 0.0)), 0.0)
    q, k, v, g = q_ref[...], k_ref[...], v_ref[...], g_ref[...]
    weight_grad = (dot(g, v, 1, 1) * decay).astype(BF16)
    weight_value = (dot(q, k, 1, 1) * decay).astype(BF16)
    iq_ref[0] = SCALE * dot(weight_grad, k, 1, 0)
    ik_ref[0] = SCALE * dot(weight_grad, q, 0, 0)
    iv_ref[0] = SCALE * dot(weight_value, g, 0, 0)


def inner_sums(ids, own, base, log_decay, *tokens):
    flops = PAIR * 5 * 2 * TOK * TOK * D
    return pl.pallas_call(
        functools.partial(inner_kernel, own, base),
        out_shape=[shaped(PAIR, TOK, D)] * 3,
        grid_spec=pltpu.PrefetchScalarGridSpec(
            num_scalar_prefetch=1,
            grid=(PAIR,),
            in_specs=[whole((HEADS, TOK))] + [head_spec(own, base)] * 4,
            out_specs=[pl.BlockSpec((1, TOK, D), lambda i, ids: (i, 0, 0))] * 3,
            scratch_shapes=[pltpu.VMEM((TOK, HEADS), F32), pltpu.VMEM((HEADS, TOK), F32)],
        ),
        compiler_params=params(),
        cost_estimate=pl.CostEstimate(
            flops=flops, transcendentals=PAIR * TOK * TOK, bytes_accessed=2 * 1024 * 1024
        ),
        name="inner_sums",
    )(ids, log_decay, *tokens)


def grads_kernel(own, base, ids, fac_ref, k_ref, v_ref, g_ref, iq_ref, ik_ref, iv_ref, *rest):
    st_ref = rest[0]
    gq_ref, gk_ref, gv_ref = rest[-3:]
    head = first_head(ids, own, base) + pl.program_id(0)
    factors = fac_ref[...]
    rising = SCALE * pick_column(factors, head)
    falling = SCALE * pick_column(factors, head + HEADS)
    k, v, g = k_ref[...], v_ref[...], g_ref[...]
    fwd = st_ref[0, 0:D, :].astype(BF16)
    rev = st_ref[0, D : 2 * D, :].astype(BF16)
    gq_ref[...] = (iq_ref[0] + rising * dot(g, fwd, 1, 1)).astype(BF16)
    gk_ref[...] = (ik_ref[0] + falling * dot(v, rev, 1, 1)).astype(BF16)
    gv_ref[...] = (iv_ref[0] + falling * dot(k, rev, 1, 0)).astype(BF16)


def gradients(ids, own, base, factors, k, v, g, inner, states, started=()):
    shape = jax.ShapeDtypeStruct((TOK, HEADS * D), BF16)
    count = len(started)
    slot = lambda rows: pl.BlockSpec((1, rows, D), lambda i, ids: (i, 0, 0))
    column = head_spec(own, base)
    return pl.pallas_call(
        functools.partial(grads_kernel, own, base),
        out_shape=[shape] * 3,
        grid_spec=pltpu.PrefetchScalarGridSpec(
            num_scalar_prefetch=1,
            grid=(PAIR,),
            in_specs=[whole((TOK, 2 * HEADS))]
            + [column] * 3
            + [slot(TOK)] * 3
            + [slot(2 * D)]
            + [pl.BlockSpec(memory_space=pl.ANY)] * count,
            out_specs=[column] * 3,
        ),
        input_output_aliases={9 + n: n for n in range(count)},
        compiler_params=params(),
        name="gradients",
    )(ids, factors, k, v, g, *inner, states, *started)


def shift_ring(value, axis, shift):
    ring = [(i, (i + shift) % RING) for i in range(RING)]
    return lax.ppermute(value, axis, ring)


def exchange(pieces, axis):
    arrived = [pieces[0], None, None, None]
    for shift in (1, 3, 2):
        arrived[(RING - shift) % RING] = shift_ring(pieces[shift], axis, shift)
    return arrived


def body(queries, keys, values, grad_out, log_decay):
    ids = jnp.stack([lax.axis_index(name) for name in ("core", "z", "y", "x")]).astype(jnp.int32)
    swap = functools.partial(lax.ppermute, axis_name="core", perm=[(0, 1), (1, 0)])
    send, factors, *tokens = load_and_start(ids, log_decay, queries, keys, values, grad_out)
    others = [swap(send)]
    others.append(swap(device_states(ids, False, PAIR, factors, *tokens)))
    owns = [device_states(ids, True, base, factors, *tokens) for base in (0, PAIR)]
    places = [(own, base) for own in (True, False) for base in (0, PAIR)]
    inner = [inner_sums(ids, own, base, log_decay, *tokens) for own, base in places]
    x_shape = [shaped(PAIR, 2 * XROWS + 8, D)] * RING
    y_shape = [shaped(PAIR, 2 * YROWS + 8, D)] * RING
    z_shape = [shaped(PAIR, YROWS + 8, D)] * (RING - 1)
    rows, keeps, arrivals = ([], [], [])
    for own, other in zip(owns, others):
        pieces = vmem_call(combine_kernel, "combine_cores", x_shape, ids, (own, other))
        rows.append(exchange(pieces, "x"))
    rows[0], inner = lax.optimization_barrier((rows[0], inner))
    for own, other, row in zip(owns, others, rows):
        pieces = vmem_call(
            row_kernel,
            "row_totals",
            y_shape,
            ids,
            row,
            [pltpu.VMEM((PAIR, 2 * XROWS + 8, D), F32)],
        )
        column = exchange(pieces, "y")
        pieces = vmem_call(plane_kernel, "plane_totals", z_shape, ids, column)
        planes = exchange([None, *pieces], "z")[1:]
        pieces = vmem_call(
            outer_kernel,
            "outer_prefixes",
            [shaped(PAIR, 2 * YROWS, D)] * RING,
            ids,
            (*planes, *column),
            [pltpu.VMEM((PAIR, 2 * YROWS, D), F32)],
        )
        returned = exchange(pieces, "y")
        pieces = vmem_call(
            chip_kernel,
            "chip_prefixes",
            [shaped(PAIR, 2 * XROWS, D)] * RING,
            ids,
            (*returned, *row),
            [pltpu.VMEM((PAIR, 2 * XROWS, D), F32)],
        )
        final = exchange(pieces, "x")
        pair = shaped(PAIR, 2 * D, D)
        operands = (*final, own, other)
        send = vmem_call(
            functools.partial(middle_kernel, False), "states_to_send", pair, ids, operands
        )
        arrivals.append(swap(send))
        keeps.append(
            vmem_call(functools.partial(middle_kernel, True), "states_to_keep", pair, ids, operands)
        )
    grads = ()
    for (own, base), sums, state in zip(places, inner, keeps + arrivals):
        grads = gradients(ids, own, base, factors, *tokens[1:], sums, state, grads)
    return tuple(grads)


def solution(mesh):
    torus = Mesh(mesh.devices.reshape(4, 4, 4, 2), ALL)
    rows = P(ALL, None)
    return jax.shard_map(
        body,
        mesh=torus,
        in_specs=(rows, rows, rows, rows, P(None, ALL)),
        out_specs=(rows, rows, rows),
        check_vma=False,
    )
```
